32 devices in a mesh: pts: 8 (over z, y), cent: 4 (over x, core).
Axes of the slice: x: 2, y: 2, z: 4, core: 2. Of those that a mesh axis runs over, the one named last changes fastest.
Arguments:
- points: bfloat16 [65536, 512], P(('pts', 'cent')), may hold values from -128 to 128
- centroids: bfloat16 [8192, 512], P('pts'), may hold values from -32 to 32
- candidates: int32 [4096, 2], P(('pts', 'cent')), may hold values from 0 to 31, all different within a row; in each aligned block of 128 rows (0 to 127, 128 to 255, ...) at most 9 rows name the same one
Outputs:
- new_centroids: bfloat16 [8192, 512], P('pts')
- point_lse: float32 [65536], P(('pts', 'cent'))
The draws below stay inside these ranges and needn't reach their ends.
Inputs may be any that keep to these rules, and one draw needn't show every extreme that they name: `candidates`: within the 128 point blocks of one device, no centroid block is named more than 9 times; the two ids of a point block differ.
All inputs are finite; a program needn't handle non-finite values.
Results may differ from the reference program's by a relative error of at most 0.006.
Values may be sent and summed in bfloat16 or wider, within the bound.
A program may use at most 64 MiB of HBM per device.

```python
import math
import jax
import jax.numpy as jnp
import numpy as np
from jax import lax

D = 512
CB = 256
PB = 16
PBD = 128
ITERS = 2
NCB = 32
K = 8192
CAP = 9
NPB = 4096
NPTS = 65536


def draw_centroids(key, part):
    values = jnp.clip(jax.random.normal(jax.random.fold_in(key, 11), (K, D), jnp.float32), -6.0, 6.0)
    return jnp.clip(values, -32.0, 32.0).astype(jnp.bfloat16)


def draw_points(key, part):
    values = jnp.clip(jax.random.normal(jax.random.fold_in(key, 17), (NPTS, D), jnp.float32), -6.0, 6.0)
    return jnp.clip(values, -128.0, 128.0).astype(jnp.bfloat16)


def deal_out(rng, own, number, rows, amount, top, reach, skew):
    ranking = jax.random.permutation(rng, amount)
    heavy_load, ordinary = shares(amount, rows * top, reach, skew, True), shares(amount, rows * top, reach, skew, False)
    places = jnp.arange(amount)

    def named(tallies, turn):
        used = int((tallies > 0).sum())
        fixed = max(1, used // 4)
        passed = fixed + (places - fixed + turn * (used - fixed)) % max(1, amount - fixed)
        return jnp.zeros((amount,), jnp.int32).at[ranking[jnp.where(places < fixed, places, passed)]].set(jnp.asarray(tallies, jnp.int32))

    tallies = jnp.where(number % 4 == 0, named(heavy_load, number // 4), named(ordinary, number - number // 4 - 1))
    mixed = jax.random.permutation(jax.random.fold_in(own, 3), amount)
    donor, receiver = mixed[0:amount // 2 * 2:2], mixed[1:amount // 2 * 2:2]
    room = jnp.minimum(tallies[donor] - 1, reach - tallies[receiver]) // 2
    room = jnp.where((donor == ranking[0]) | (receiver == ranking[0]) | (tallies[receiver] == 0), 0, jnp.maximum(room, 0))
    passed = jax.random.randint(jax.random.fold_in(own, 4), (amount // 2,), 0, 1 << 20) % (room + 1)
    tallies = tallies.at[donor].add(-passed).at[receiver].add(passed)
    items = jnp.searchsorted(jnp.cumsum(tallies), jnp.arange(rows * top), side="right").astype(jnp.int32)
    grid = items.reshape(top, rows).T
    grid = grid[jax.random.permutation(jax.random.fold_in(own, 1), rows)]
    turn = jax.random.randint(jax.random.fold_in(own, 2), (rows, 1), 0, top)
    return jnp.take_along_axis(grid, (jnp.arange(top)[None, :] + turn) % top, axis=1)


def shares(number_of, total, limit, lean, full):
    loads = [(1 << 20) // math.isqrt(standing ** lean) + 1 for standing in range(1, number_of + 1)]
    largest = limit if full else min(limit, max(-(-total // number_of), total * loads[0] // sum(loads)))
    least = 1 if total - largest >= number_of - 1 else 0
    holding, surplus = [largest] + [least] * (number_of - 1), total - largest - least * (number_of - 1)
    while surplus > 0:
        free = [i for i in range(1, number_of) if holding[i] < largest] or [i for i in range(1, number_of) if holding[i] < limit]
        pool, budget = sum([loads[i] for i in free]), surplus
        for i in free:
            extra = min(limit - holding[i], max(1, budget * loads[i] // pool), surplus)
            holding[i] = holding[i] + extra
            surplus = surplus - extra
    return np.array(holding)


def setup_inputs(seed: int = 0) -> dict:
    key_list = jax.random.split(jax.random.key(seed), 4)
    points = draw_points(jax.random.fold_in(key_list[3], 71), 0)
    centroids = draw_centroids(jax.random.fold_in(key_list[3], 71), 0)
    candidates_keys = jax.random.split(jax.random.fold_in(key_list[2], 1), NPB // PBD)
    candidates_turns = jax.random.permutation(jax.random.fold_in(key_list[2], 3), NPB // PBD)
    candidates = jax.vmap(lambda own, number: deal_out(jax.random.fold_in(key_list[2], 2), own, number, PBD, NCB, 2, CAP, 2))(candidates_keys, candidates_turns).reshape((NPB, 2))
    return dict(points=points, centroids=centroids, candidates=candidates)


def stable_lse(scores, reduce_axis):
    highest = lax.optimization_barrier(jnp.max(scores, axis=reduce_axis, keepdims=True))
    summed = lax.optimization_barrier(jnp.sum(jnp.exp(scores - highest), axis=reduce_axis))
    return jnp.squeeze(highest, reduce_axis) + jnp.log(summed)

def em_round(points, current, candidates):
    inverse_root = 1.0 / math.sqrt(D)
    group_count = candidates.shape[0] // PBD
    grouped = points.reshape(group_count, PBD, PB, D)
    picked = candidates.reshape(group_count, PBD, 2)
    centre_table = current.reshape(NCB, CB, D)
    centre_norms = lax.optimization_barrier(jnp.sum(jnp.square(centre_table.astype(jnp.float32)), axis=2))

    def visit_group(running, element):
        weighted, masses = running
        group_rows, group_ids = element
        chosen = centre_table[group_ids].astype(jnp.float32)
        products = jnp.einsum('gpd,gjmd->gjpm', group_rows.astype(jnp.float32), chosen)
        scores = inverse_root * (2.0 * products - centre_norms[group_ids][:, :, None, :])
        partial_value = stable_lse(scores, 3)
        point_lse = stable_lse(partial_value, 1)
        weights = jnp.exp(scores - point_lse[:, None, :, None])
        rounded = lax.optimization_barrier(weights.astype(jnp.bfloat16)).astype(jnp.float32)
        contribution = jnp.einsum('gjpm,gpd->gjmd', rounded, group_rows.astype(jnp.float32))
        weighted = weighted.at[group_ids].add(contribution)
        masses = masses.at[group_ids].add(lax.optimization_barrier(jnp.sum(weights, axis=2)))
        return ((weighted, masses), point_lse)
    start_sums = jnp.zeros((NCB, CB, D), jnp.float32)
    start_mass = jnp.zeros((NCB, CB), jnp.float32)
    (weighted, masses), point_lse = lax.scan(visit_group, (start_sums, start_mass), (grouped, picked))
    return (weighted.reshape(K, D), masses.reshape(K), point_lse.reshape(-1))

def reference(points, centroids, candidates):
    current = centroids
    point_lse = jnp.zeros((NPTS,), jnp.float32)
    for iteration in range(ITERS):
        weighted, masses, point_lse = em_round(points, current, candidates)
        current = ((weighted + current.astype(jnp.float32)) / (masses[:, None] + 1.0)).astype(jnp.bfloat16)
    return (current, point_lse)
```

```python
import math

import jax
import jax.numpy as jnp
from jax import lax
from jax.sharding import PartitionSpec as P

CB = 256
PB = 16
ITERS = 2


def stable_lse(scores, reduce_axis):
    highest = jnp.max(scores, axis=reduce_axis, keepdims=True)
    summed = jnp.sum(jnp.exp(scores - highest), axis=reduce_axis)
    return jnp.squeeze(highest, reduce_axis) + jnp.log(summed)


def make_scoring(centre_table, centre_norms, inverse_root):

    def scoring(package):
        slot_rows, slot_flags = package
        leading = slot_rows.shape[0]
        flat_rows = slot_rows.reshape(leading, -1, slot_rows.shape[-1])
        products = jnp.einsum(
            "lsd,lmd->lsm", flat_rows, centre_table, preferred_element_type=jnp.float32
        )
        scores = inverse_root * (2.0 * products - centre_norms[:, None, :])
        scores = scores.reshape(slot_rows.shape[:-1] + (centre_table.shape[1],))
        return (slot_rows, slot_flags, scores, stable_lse(scores, scores.ndim - 1))

    return scoring


def on_device(points, centroids, candidates):
    feature_width = points.shape[1]
    inverse_root = 1.0 / math.sqrt(feature_width)
    owners = lax.axis_size("pts")
    held_blocks = centroids.shape[0] // CB
    point_blocks = candidates.shape[0]
    total_blocks = held_blocks * owners
    capacity = max(2, 2 * point_blocks // total_blocks + 1)
    slot_count = held_blocks * owners * capacity
    grouped = points.reshape(point_blocks, PB, feature_width)
    picked = candidates.reshape(-1)
    entry_count = picked.shape[0]
    labels = jnp.arange(total_blocks, dtype=jnp.int32)
    member = (picked[:, None] == labels[None, :]).astype(jnp.bfloat16)
    entry_index = jnp.arange(entry_count, dtype=jnp.int32)
    earlier = (entry_index[None, :] < entry_index[:, None]).astype(jnp.bfloat16)
    prior_hits = jnp.dot(earlier, member, preferred_element_type=jnp.float32)
    arrival = jnp.sum(prior_hits * member.astype(jnp.float32), axis=1).astype(jnp.int32)
    local_block = picked % held_blocks
    target = picked // held_blocks
    position = (local_block * owners + target) * capacity + arrival
    slot_shape = (held_blocks, owners, capacity)
    current = centroids
    places = jnp.arange(slot_count, dtype=jnp.int32)
    source = (
        jnp.sum(
            jnp.where(position[:, None] == places[None, :], entry_index[:, None] + 1, 0), axis=0
        )
        - 1
    )
    filled = source >= 0
    home_block = jnp.maximum(source, 0) // 2
    outgoing = jnp.where(filled[:, None, None], grouped[home_block], jnp.zeros((), jnp.bfloat16))
    outgoing = outgoing.reshape(slot_shape + (PB, feature_width))
    slot_marks = jnp.broadcast_to(filled[:, None], (slot_count, PB)).astype(jnp.bfloat16)
    slot_marks = slot_marks.reshape(slot_shape + (PB,))
    point_lse = jnp.zeros((point_blocks, PB), jnp.float32)
    arrived = lax.all_to_all(outgoing, "pts", split_axis=1, concat_axis=1, tiled=True)
    arrived_marks = lax.all_to_all(slot_marks, "pts", split_axis=1, concat_axis=1, tiled=True)
    for iteration in range(ITERS):
        centre_table = current.reshape(-1, CB, feature_width)
        centre_norms = jnp.sum(jnp.square(centre_table.astype(jnp.float32)), axis=2)
        scoring = make_scoring(centre_table, centre_norms, inverse_root)
        arrived, arrived_marks, scores, partial_value = scoring(
            (arrived, arrived_marks)
        )
        returned = lax.all_to_all(partial_value, "pts", split_axis=1, concat_axis=1, tiled=True)
        per_entry = returned.reshape(slot_count, PB)[position]
        paired = per_entry.reshape(point_blocks, 2, PB)
        point_lse = stable_lse(paired, 1)
        outward = jnp.where(filled[:, None], point_lse[home_block], jnp.zeros((), jnp.float32))
        outward = outward.reshape(slot_shape + (PB,))
        inward = lax.all_to_all(outward, "pts", split_axis=1, concat_axis=1, tiled=True)
        weights = jnp.exp(scores - inward[..., None]) * arrived_marks.astype(jnp.float32)[..., None]
        leading = weights.shape[0]
        flat_weights = weights.reshape(leading, -1, CB)
        masses = jnp.sum(flat_weights, axis=1).reshape(leading * CB)
        rounded = flat_weights.astype(jnp.bfloat16)
        flat_rows = arrived.reshape(leading, -1, feature_width)
        weighted = jnp.einsum(
            "lsm,lsd->lmd", rounded, flat_rows, preferred_element_type=jnp.float32
        )
        weighted = weighted.reshape(leading * CB, feature_width)
        share_sums, share_mass = (
            lax.psum_scatter(weighted, "cent", scatter_dimension=0, tiled=True),
            lax.psum_scatter(masses, "cent", scatter_dimension=0, tiled=True),
        )
        share_rows = share_sums.shape[0]
        first_row = lax.axis_index("cent") * share_rows
        previous = lax.dynamic_slice_in_dim(current, first_row, share_rows, 0).astype(jnp.float32)
        renewed = ((share_sums + previous) / (share_mass[:, None] + 1.0)).astype(jnp.bfloat16)
        current = lax.all_gather(renewed, "cent", axis=0, tiled=True)
    return (current, point_lse.reshape(-1))


def solution(mesh):
    return jax.shard_map(
        on_device,
        mesh=mesh,
        in_specs=(P(("pts", "cent"), None), P("pts", None), P(("pts", "cent"), None)),
        out_specs=(P("pts", None), P(("pts", "cent"))),
        check_vma=False,
    )
```

```python
import functools
import math

import jax
import jax.numpy as jnp
from jax import lax
from jax.experimental import pallas as pl
from jax.experimental.pallas import tpu as pltpu
from jax.sharding import PartitionSpec as P

CB = 256
PB = 16
ITERS = 2


def stable_lse(scores, reduce_axis):
    highest = jnp.max(scores, axis=reduce_axis, keepdims=True)
    summed = jnp.sum(jnp.exp(scores - highest), axis=reduce_axis)
    return jnp.squeeze(highest, reduce_axis) + jnp.log(summed)


def make_scoring(centre_table, centre_norms, inverse_root):

    def scoring(package):
        slot_rows, slot_flags = package
        leading = slot_rows.shape[0]
        flat_rows = slot_rows.reshape(leading, -1, slot_rows.shape[-1])
        products = jnp.einsum(
            "lsd,lmd->lsm", flat_rows, centre_table, preferred_element_type=jnp.float32
        )
        scores = inverse_root * (2.0 * products - centre_norms[:, None, :])
        scores = scores.reshape(slot_rows.shape[:-1] + (centre_table.shape[1],))
        return (slot_rows, slot_flags, scores, stable_lse(scores, scores.ndim - 1))

    return scoring


def exchange_points(points, centroids, candidates):
    feature_width = points.shape[1]
    inverse_root = 1.0 / math.sqrt(feature_width)
    owners = lax.axis_size("pts")
    held_blocks = centroids.shape[0] // CB
    point_blocks = candidates.shape[0]
    total_blocks = held_blocks * owners
    capacity = max(2, 2 * point_blocks // total_blocks + 1)
    slot_count = held_blocks * owners * capacity
    grouped = points.reshape(point_blocks, PB, feature_width)
    picked = candidates.reshape(-1)
    entry_count = picked.shape[0]
    labels = jnp.arange(total_blocks, dtype=jnp.int32)
    member = (picked[:, None] == labels[None, :]).astype(jnp.bfloat16)
    entry_index = jnp.arange(entry_count, dtype=jnp.int32)
    earlier = (entry_index[None, :] < entry_index[:, None]).astype(jnp.bfloat16)
    prior_hits = jnp.dot(earlier, member, preferred_element_type=jnp.float32)
    arrival = jnp.sum(prior_hits * member.astype(jnp.float32), axis=1).astype(jnp.int32)
    local_block = picked % held_blocks
    target = picked // held_blocks
    position = (local_block * owners + target) * capacity + arrival
    slot_shape = (held_blocks, owners, capacity)
    current = centroids
    places = jnp.arange(slot_count, dtype=jnp.int32)
    source = (
        jnp.sum(
            jnp.where(position[:, None] == places[None, :], entry_index[:, None] + 1, 0), axis=0
        )
        - 1
    )
    filled = source >= 0
    home_block = jnp.maximum(source, 0) // 2
    outgoing = jnp.where(filled[:, None, None], grouped[home_block], jnp.zeros((), jnp.bfloat16))
    outgoing = outgoing.reshape(slot_shape + (PB, feature_width))
    slot_marks = jnp.broadcast_to(filled[:, None], (slot_count, PB)).astype(jnp.bfloat16)
    slot_marks = slot_marks.reshape(slot_shape + (PB,))
    point_lse = jnp.zeros((point_blocks, PB), jnp.float32)
    arrived = lax.all_to_all(outgoing, "pts", split_axis=1, concat_axis=1, tiled=True)
    arrived_marks = lax.all_to_all(slot_marks, "pts", split_axis=1, concat_axis=1, tiled=True)
    for iteration in range(ITERS):
        centre_table = current.reshape(-1, CB, feature_width)
        centre_norms = jnp.sum(jnp.square(centre_table.astype(jnp.float32)), axis=2)
        scoring = make_scoring(centre_table, centre_norms, inverse_root)
        arrived, arrived_marks, scores, partial_value = scoring(
            (arrived, arrived_marks)
        )
        returned = lax.all_to_all(partial_value, "pts", split_axis=1, concat_axis=1, tiled=True)
        per_entry = returned.reshape(slot_count, PB)[position]
        paired = per_entry.reshape(point_blocks, 2, PB)
        point_lse = stable_lse(paired, 1)
        outward = jnp.where(filled[:, None], point_lse[home_block], jnp.zeros((), jnp.float32))
        outward = outward.reshape(slot_shape + (PB,))
        inward = lax.all_to_all(outward, "pts", split_axis=1, concat_axis=1, tiled=True)
        weights = jnp.exp(scores - inward[..., None]) * arrived_marks.astype(jnp.float32)[..., None]
        leading = weights.shape[0]
        flat_weights = weights.reshape(leading, -1, CB)
        masses = jnp.sum(flat_weights, axis=1).reshape(leading * CB)
        rounded = flat_weights.astype(jnp.bfloat16)
        flat_rows = arrived.reshape(leading, -1, feature_width)
        weighted = jnp.einsum(
            "lsm,lsd->lmd", rounded, flat_rows, preferred_element_type=jnp.float32
        )
        weighted = weighted.reshape(leading * CB, feature_width)
        share_sums, share_mass = (
            lax.psum_scatter(weighted, "cent", scatter_dimension=0, tiled=True),
            lax.psum_scatter(masses, "cent", scatter_dimension=0, tiled=True),
        )
        share_rows = share_sums.shape[0]
        first_row = lax.axis_index("cent") * share_rows
        previous = lax.dynamic_slice_in_dim(current, first_row, share_rows, 0).astype(jnp.float32)
        renewed = ((share_sums + previous) / (share_mass[:, None] + 1.0)).astype(jnp.bfloat16)
        current = lax.all_gather(renewed, "cent", axis=0, tiled=True)
    return (current, point_lse.reshape(-1))


def em_kernel(
    blocks, capacity, inverse_root, source, points, table, sums, masses, lse_out,
    rows_held, score_held, partial_held, lse_held,
):
    width = table.shape[1]
    group = capacity * PB
    entries = partial_held.shape[0] - 1
    point_blocks = entries // 2
    ones = jnp.ones((8, width), jnp.bfloat16)
    across = (((1,), (1,)), ((), ()))

    @pl.loop(0, blocks)
    def _(b):
        for c in range(capacity):
            home = jnp.maximum(source[b * capacity + c], 0) // 2
            rows_held[b, pl.ds(c * PB, PB), :] = points[home]
        centre = table[pl.ds(pl.multiple_of(b * CB, CB), CB), :]
        wide = centre.astype(jnp.float32)
        square = wide * wide
        high = square.astype(jnp.bfloat16)
        low = (square - high.astype(jnp.float32)).astype(jnp.bfloat16)
        norms = lax.dot_general(ones, high, across, preferred_element_type=jnp.float32)
        norms += lax.dot_general(ones, low, across, preferred_element_type=jnp.float32)
        products = lax.dot_general(
            rows_held[b], centre, across, preferred_element_type=jnp.float32
        )
        scores = inverse_root * (2.0 * products - norms[0:1, :])
        highest = jnp.max(scores, axis=1, keepdims=True)
        partial = highest + jnp.log(jnp.sum(jnp.exp(scores - highest), axis=1, keepdims=True))
        partial = jnp.broadcast_to(partial, (group, 128))
        score_held[b] = scores
        for c in range(capacity):
            entry = source[b * capacity + c]
            partial_held[jnp.where(entry < 0, entries, entry)] = partial[c * PB : (c + 1) * PB]

    @pl.loop(0, point_blocks // 8)
    def _(i):
        for j in range(8):
            g = i * 8 + j
            first, second = partial_held[2 * g], partial_held[2 * g + 1]
            highest = jnp.maximum(first, second)
            value = highest + jnp.log(jnp.exp(first - highest) + jnp.exp(second - highest))
            lse_held[g] = value
            lse_out[g] = value

    lse_held[point_blocks] = jnp.full((PB, 128), 1e30, jnp.float32)

    @pl.loop(0, blocks)
    def _(b):
        taken = []
        for c in range(capacity):
            entry = source[b * capacity + c]
            taken.append(lse_held[jnp.where(entry < 0, point_blocks, entry // 2)])
        lse = jnp.concatenate(taken, axis=0)
        lse = jnp.concatenate([lse] * (CB // 128), axis=1)
        weights = jnp.exp(score_held[b] - lse)
        masses[b] = jnp.sum(weights, axis=0, keepdims=True)
        total = lax.dot_general(
            weights.astype(jnp.bfloat16), rows_held[b], (((0,), (0,)), ((), ())),
            preferred_element_type=jnp.float32,
        )
        sums[pl.ds(pl.multiple_of(b * CB, CB), CB), :] = total.astype(sums.dtype)


def exchange_centroids(points, centroids, candidates):
    width = points.shape[1]
    axes = ("pts", "cent")
    devices = lax.axis_size("pts") * lax.axis_size("cent")
    point_blocks = candidates.shape[0]
    total_rows = centroids.shape[0] * lax.axis_size("pts")
    blocks = total_rows // CB
    capacity = max(2, 2 * point_blocks // blocks + 1)
    entries = 2 * point_blocks
    picked = candidates.reshape(-1)
    labels = jnp.arange(blocks, dtype=jnp.int32)
    member = (picked[:, None] == labels[None, :]).astype(jnp.bfloat16)
    entry_index = jnp.arange(entries, dtype=jnp.int32)
    earlier = (entry_index[None, :] < entry_index[:, None]).astype(jnp.bfloat16)
    prior_hits = jnp.dot(earlier, member, preferred_element_type=jnp.float32)
    arrival = jnp.sum(prior_hits * member.astype(jnp.float32), axis=1).astype(jnp.int32)
    position = picked * capacity + arrival
    places = jnp.arange(blocks * capacity, dtype=jnp.int32)
    source = (
        jnp.sum(
            jnp.where(position[:, None] == places[None, :], entry_index[:, None] + 1, 0), axis=0
        )
        - 1
    )
    group = capacity * PB
    vmem = pl.BlockSpec(memory_space=pltpu.VMEM)
    round_call = pl.pallas_call(
        functools.partial(em_kernel, blocks, capacity, 1.0 / math.sqrt(width)),
        out_shape=(
            jax.ShapeDtypeStruct((total_rows, width), jnp.bfloat16),
            jax.ShapeDtypeStruct((blocks, 1, CB), jnp.float32),
            jax.ShapeDtypeStruct((point_blocks, PB, 128), jnp.float32),
        ),
        in_specs=[pl.BlockSpec(memory_space=pltpu.SMEM), vmem, vmem],
        out_specs=(vmem, vmem, vmem),
        scratch_shapes=[
            pltpu.VMEM((blocks, group, width), jnp.bfloat16),
            pltpu.VMEM((blocks, group, CB), jnp.float32),
            pltpu.VMEM((entries + 1, PB, 128), jnp.float32),
            pltpu.VMEM((point_blocks + 1, PB, 128), jnp.float32),
        ],
        compiler_params=pltpu.CompilerParams(vmem_limit_bytes=50 << 20),
    )
    grouped = points.reshape(point_blocks, PB, width)
    share_rows = total_rows // devices
    share = lax.dynamic_slice_in_dim(
        centroids, lax.axis_index("cent") * share_rows, share_rows, 0
    )
    for iteration in range(ITERS):
        table = lax.all_gather(share, axes, axis=0, tiled=True)
        sums, masses, lse = round_call(source, grouped, table)
        share_sums = lax.psum_scatter(sums, axes, scatter_dimension=0, tiled=True)
        share_mass = lax.psum_scatter(
            masses.reshape(total_rows), axes, scatter_dimension=0, tiled=True
        )
        share = (share_sums.astype(jnp.float32) + share.astype(jnp.float32)) / (
            share_mass[:, None] + 1.0
        )
        share = share.astype(jnp.bfloat16)
    return (lax.all_gather(share, "cent", axis=0, tiled=True), lse[:, :, 0].reshape(-1))


def on_device(points, centroids, candidates):
    width = points.shape[1]
    table_size = centroids.shape[0] * lax.axis_size("pts") * width
    blocks = table_size // width // CB
    slots = blocks * max(2, 2 * candidates.shape[0] // blocks + 1)
    held = 4 * table_size + 2 * points.size + slots * PB * (2 * width + 4 * CB)
    if held <= 40 << 20 and candidates.shape[0] % 8 == 0:
        return exchange_centroids(points, centroids, candidates)
    return exchange_points(points, centroids, candidates)


def solution(mesh):
    return jax.shard_map(
        on_device,
        mesh=mesh,
        in_specs=(P(("pts", "cent"), None), P("pts", None), P(("pts", "cent"), None)),
        out_specs=(P("pts", None), P(("pts", "cent"))),
        check_vma=False,
    )
```

```python
import math

import jax
import jax.numpy as jnp
from jax import lax
from jax.experimental import pallas as pl
from jax.experimental.pallas import tpu as pltpu
from jax.sharding import PartitionSpec as P

CB = 256
PB = 16
ITERS = 2


def stable_lse(scores, reduce_axis):
    highest = jnp.max(scores, axis=reduce_axis, keepdims=True)
    summed = jnp.sum(jnp.exp(scores - highest), axis=reduce_axis)
    return jnp.squeeze(highest, reduce_axis) + jnp.log(summed)


def pick_kernel(home_block, grouped, outgoing):
    @pl.loop(0, outgoing.shape[0])
    def _(slot):
        outgoing[slot] = grouped[home_block[slot]]


def pick_blocks(home_block, grouped):
    vmem = pl.BlockSpec(memory_space=pltpu.VMEM)
    return pl.pallas_call(
        pick_kernel,
        out_shape=jax.ShapeDtypeStruct(home_block.shape + grouped.shape[1:], grouped.dtype),
        in_specs=[pl.BlockSpec(memory_space=pltpu.SMEM), vmem],
        out_specs=vmem,
        compiler_params=pltpu.CompilerParams(vmem_limit_bytes=32 << 20),
    )(home_block, grouped)


def make_scoring(centre_table, centre_norms, inverse_root):

    def scoring(package):
        slot_rows = package
        leading = slot_rows.shape[0]
        flat_rows = slot_rows.reshape(leading, -1, slot_rows.shape[-1])
        products = jnp.einsum(
            "lsd,lmd->lsm", flat_rows, centre_table, preferred_element_type=jnp.float32
        )
        scores = inverse_root * (2.0 * products - centre_norms[:, None, :])
        scores = scores.reshape(slot_rows.shape[:-1] + (centre_table.shape[1],))
        return (scores, stable_lse(scores, scores.ndim - 1))

    return scoring


def on_device(points, centroids, candidates):
    feature_width = points.shape[1]
    inverse_root = 1.0 / math.sqrt(feature_width)
    owners = lax.axis_size("pts")
    held_blocks = centroids.shape[0] // CB
    point_blocks = candidates.shape[0]
    total_blocks = held_blocks * owners
    capacity = max(2, 2 * point_blocks // total_blocks + 1)
    slot_count = held_blocks * owners * capacity
    grouped = points.reshape(point_blocks, PB, feature_width)
    picked = candidates.reshape(-1)
    entry_count = picked.shape[0]
    labels = jnp.arange(total_blocks, dtype=jnp.int32)
    member = (picked[:, None] == labels[None, :]).astype(jnp.bfloat16)
    entry_index = jnp.arange(entry_count, dtype=jnp.int32)
    earlier = (entry_index[None, :] < entry_index[:, None]).astype(jnp.bfloat16)
    prior_hits = jnp.dot(earlier, member, preferred_element_type=jnp.float32)
    arrival = jnp.sum(prior_hits * member.astype(jnp.float32), axis=1).astype(jnp.int32)
    local_block = picked % held_blocks
    target = picked // held_blocks
    position = (local_block * owners + target) * capacity + arrival
    slot_shape = (held_blocks, owners, capacity)
    current = centroids
    places = jnp.arange(slot_count, dtype=jnp.int32)
    source = (
        jnp.sum(
            jnp.where(position[:, None] == places[None, :], entry_index[:, None] + 1, 0), axis=0
        )
        - 1
    )
    filled = source >= 0
    home_block = jnp.maximum(source, 0) // 2
    outgoing = pick_blocks(home_block, grouped)
    outgoing = outgoing.reshape(slot_shape + (PB, feature_width))
    point_lse = jnp.zeros((point_blocks, PB), jnp.float32)
    arrived = lax.all_to_all(outgoing, "pts", split_axis=1, concat_axis=1, tiled=True)
    for iteration in range(ITERS):
        centre_table = current.reshape(-1, CB, feature_width)
        centre_norms = jnp.sum(jnp.square(centre_table.astype(jnp.float32)), axis=2)
        scoring = make_scoring(centre_table, centre_norms, inverse_root)
        scores, partial_value = scoring(arrived)
        returned = lax.all_to_all(partial_value, "pts", split_axis=1, concat_axis=1, tiled=True)
        per_entry = returned.reshape(slot_count, PB)[position]
        paired = per_entry.reshape(point_blocks, 2, PB)
        point_lse = stable_lse(paired, 1)
        outward = jnp.where(filled[:, None], point_lse[home_block], jnp.float32(1e30))
        outward = outward.reshape(slot_shape + (PB,))
        inward = lax.all_to_all(outward, "pts", split_axis=1, concat_axis=1, tiled=True)
        weights = jnp.exp(scores - inward[..., None])
        leading = weights.shape[0]
        flat_weights = weights.reshape(leading, -1, CB)
        masses = jnp.sum(flat_weights, axis=1).reshape(leading * CB)
        rounded = flat_weights.astype(jnp.bfloat16)
        flat_rows = arrived.reshape(leading, -1, feature_width)
        weighted = jnp.einsum(
            "lsm,lsd->lmd", rounded, flat_rows, preferred_element_type=jnp.float32
        )
        weighted = weighted.astype(jnp.bfloat16).reshape(leading * CB, feature_width)
        share_sums, share_mass = (
            lax.psum_scatter(weighted, "cent", scatter_dimension=0, tiled=True),
            lax.psum_scatter(masses, "cent", scatter_dimension=0, tiled=True),
        )
        share_rows = share_sums.shape[0]
        first_row = lax.axis_index("cent") * share_rows
        previous = lax.dynamic_slice_in_dim(current, first_row, share_rows, 0).astype(jnp.float32)
        renewed = ((share_sums.astype(jnp.float32) + previous) / (share_mass[:, None] + 1.0)).astype(jnp.bfloat16)
        current = lax.all_gather(renewed, "cent", axis=0, tiled=True)
    return (current, point_lse.reshape(-1))


def solution(mesh):
    return jax.shard_map(
        on_device,
        mesh=mesh,
        in_specs=(P(("pts", "cent"), None), P("pts", None), P(("pts", "cent"), None)),
        out_specs=(P("pts", None), P(("pts", "cent"))),
        check_vma=False,
    )
```

```python
import functools
import math

import jax
import jax.numpy as jnp
from jax import lax
from jax.experimental import pallas as pl
from jax.experimental.pallas import tpu as pltpu
from jax.sharding import PartitionSpec as P

CB = 256
PB = 16
ITERS = 2


def stable_lse(scores, reduce_axis):
    highest = jnp.max(scores, axis=reduce_axis, keepdims=True)
    summed = jnp.sum(jnp.exp(scores - highest), axis=reduce_axis)
    return jnp.squeeze(highest, reduce_axis) + jnp.log(summed)


def pick_kernel(home_block, grouped, outgoing):
    @pl.loop(0, outgoing.shape[0])
    def _(slot):
        outgoing[slot] = grouped[home_block[slot]]


def pick_blocks(home_block, grouped):
    vmem = pl.BlockSpec(memory_space=pltpu.VMEM)
    return pl.pallas_call(
        pick_kernel,
        out_shape=jax.ShapeDtypeStruct(home_block.shape + grouped.shape[1:], grouped.dtype),
        in_specs=[pl.BlockSpec(memory_space=pltpu.SMEM), vmem],
        out_specs=vmem,
        compiler_params=pltpu.CompilerParams(vmem_limit_bytes=32 << 20),
    )(home_block, grouped)


def swap_kernel(parts, x, out, landed, send_sem, recv_sem):
    me = lax.axis_index("pts")
    barrier = pltpu.get_barrier_semaphore()
    for step in range(1, parts):
        pl.semaphore_signal(
            barrier, inc=1, device_id={"pts": lax.rem(me + step, parts)},
            device_id_type=pl.DeviceIdType.MESH,
        )
    pl.semaphore_wait(barrier, parts - 1)
    copies = []
    for step in range(1, parts):
        peer = lax.rem(me + step, parts)
        copy = pltpu.make_async_remote_copy(
            src_ref=x.at[peer],
            dst_ref=landed.at[me],
            send_sem=send_sem.at[step],
            recv_sem=recv_sem.at[step],
            device_id={"pts": peer},
            device_id_type=pl.DeviceIdType.MESH,
        )
        copy.start()
        copies.append(copy)
    out[me] = x[me]
    for step in range(1, parts):
        copies[step - 1].wait()
        origin = lax.rem(me - step + parts, parts)
        out[origin] = landed[origin]


def swap(values, number):
    held, owners, capacity, width = values.shape
    size = held * capacity * width
    full = -(-size // 1024) * 1024
    flat = jnp.swapaxes(values, 0, 1).reshape(owners, size)
    flat = jnp.pad(flat, ((0, 0), (0, full - size))).reshape(owners, full // 128, 128)
    vmem = pl.BlockSpec(memory_space=pltpu.VMEM)
    result = pl.pallas_call(
        functools.partial(swap_kernel, owners),
        out_shape=jax.ShapeDtypeStruct(flat.shape, flat.dtype),
        in_specs=[vmem],
        out_specs=vmem,
        scratch_shapes=[
            pltpu.VMEM(flat.shape, flat.dtype),
            pltpu.SemaphoreType.DMA((owners,)),
            pltpu.SemaphoreType.DMA((owners,)),
        ],
        compiler_params=pltpu.CompilerParams(collective_id=number, has_side_effects=True),
    )(flat)
    result = result.reshape(owners, full)[:, :size]
    return jnp.swapaxes(result.reshape(owners, held, capacity, width), 0, 1)


def make_scoring(centre_table, centre_norms, inverse_root):

    def scoring(package):
        slot_rows = package
        leading = slot_rows.shape[0]
        flat_rows = slot_rows.reshape(leading, -1, slot_rows.shape[-1])
        products = jnp.einsum(
            "lsd,lmd->lsm", flat_rows, centre_table, preferred_element_type=jnp.float32
        )
        scores = inverse_root * (2.0 * products - centre_norms[:, None, :])
        scores = scores.reshape(slot_rows.shape[:-1] + (centre_table.shape[1],))
        return (scores, stable_lse(scores, scores.ndim - 1))

    return scoring


def on_device(points, centroids, candidates):
    feature_width = points.shape[1]
    inverse_root = 1.0 / math.sqrt(feature_width)
    owners = lax.axis_size("pts")
    held_blocks = centroids.shape[0] // CB
    point_blocks = candidates.shape[0]
    total_blocks = held_blocks * owners
    capacity = max(2, 2 * point_blocks // total_blocks + 1)
    slot_count = held_blocks * owners * capacity
    grouped = points.reshape(point_blocks, PB, feature_width)
    picked = candidates.reshape(-1)
    entry_count = picked.shape[0]
    labels = jnp.arange(total_blocks, dtype=jnp.int32)
    member = (picked[:, None] == labels[None, :]).astype(jnp.bfloat16)
    entry_index = jnp.arange(entry_count, dtype=jnp.int32)
    earlier = (entry_index[None, :] < entry_index[:, None]).astype(jnp.bfloat16)
    prior_hits = jnp.dot(earlier, member, preferred_element_type=jnp.float32)
    arrival = jnp.sum(prior_hits * member.astype(jnp.float32), axis=1).astype(jnp.int32)
    local_block = picked % held_blocks
    target = picked // held_blocks
    position = (local_block * owners + target) * capacity + arrival
    slot_shape = (held_blocks, owners, capacity)
    current = centroids
    places = jnp.arange(slot_count, dtype=jnp.int32)
    source = (
        jnp.sum(
            jnp.where(position[:, None] == places[None, :], entry_index[:, None] + 1, 0), axis=0
        )
        - 1
    )
    filled = source >= 0
    home_block = jnp.maximum(source, 0) // 2
    outgoing = pick_blocks(home_block, grouped)
    outgoing = outgoing.reshape(slot_shape + (PB, feature_width))
    point_lse = jnp.zeros((point_blocks, PB), jnp.float32)
    arrived = lax.all_to_all(outgoing, "pts", split_axis=1, concat_axis=1, tiled=True)
    for iteration in range(ITERS):
        centre_table = current.reshape(-1, CB, feature_width)
        centre_norms = jnp.sum(jnp.square(centre_table.astype(jnp.float32)), axis=2)
        scoring = make_scoring(centre_table, centre_norms, inverse_root)
        scores, partial_value = scoring(arrived)
        returned = swap(partial_value, 2 * iteration)
        per_entry = returned.reshape(slot_count, PB)[position]
        paired = per_entry.reshape(point_blocks, 2, PB)
        point_lse = stable_lse(paired, 1)
        outward = jnp.where(filled[:, None], point_lse[home_block], jnp.float32(1e30))
        outward = outward.reshape(slot_shape + (PB,))
        inward = swap(outward, 2 * iteration + 1)
        weights = jnp.exp(scores - inward[..., None])
        leading = weights.shape[0]
        flat_weights = weights.reshape(leading, -1, CB)
        masses = jnp.sum(flat_weights, axis=1).reshape(leading * CB)
        rounded = flat_weights.astype(jnp.bfloat16)
        flat_rows = arrived.reshape(leading, -1, feature_width)
        weighted = jnp.einsum(
            "lsm,lsd->lmd", rounded, flat_rows, preferred_element_type=jnp.float32
        )
        weighted = weighted.astype(jnp.bfloat16).reshape(leading * CB, feature_width)
        share_sums, share_mass = (
            lax.psum_scatter(weighted, "cent", scatter_dimension=0, tiled=True),
            lax.psum_scatter(masses, "cent", scatter_dimension=0, tiled=True),
        )
        share_rows = share_sums.shape[0]
        first_row = lax.axis_index("cent") * share_rows
        previous = lax.dynamic_slice_in_dim(current, first_row, share_rows, 0).astype(jnp.float32)
        renewed = ((share_sums.astype(jnp.float32) + previous) / (share_mass[:, None] + 1.0)).astype(jnp.bfloat16)
        current = lax.all_gather(renewed, "cent", axis=0, tiled=True)
    return (current, point_lse.reshape(-1))


def solution(mesh):
    return jax.shard_map(
        on_device,
        mesh=mesh,
        in_specs=(P(("pts", "cent"), None), P("pts", None), P(("pts", "cent"), None)),
        out_specs=(P("pts", None), P(("pts", "cent"))),
        check_vma=False,
    )
```
